32 devices in a mesh: dp: 16 (over z, x, core), mp: 2 (over y).
Axes of the slice: x: 2, y: 2, z: 4, core: 2. Of those that a mesh axis runs over, the one named last changes fastest.
Arguments:
- patches: bfloat16 [12544, 768], P(('dp', 'mp')), may hold values from -6 to 6
- captions: bfloat16 [4096, 768], P(('dp', 'mp')), may hold values from -6 to 6
- patch_image: int32 [12544], P('dp'), may hold values from 0 to 3, as said below
- caption_image: int32 [32], P('dp'), may hold values from 0 to 3, as said below
- image_norm: float32 [768], replicated, may hold values from 0.5 to 1.5
- image_ffnorm: float32 [768], replicated, may hold values from 0.5 to 1.5
- text_norm: float32 [768], replicated, may hold values from 0.5 to 1.5
- cross_norm: float32 [768], replicated, may hold values from 0.5 to 1.5
- text_ffnorm: float32 [768], replicated, may hold values from 0.5 to 1.5
- image_proj: bfloat16 [768, 2304], P(None, 'mp'), may hold values from -0.21875 to 0.21875
- image_mix: bfloat16 [768, 768], P('mp'), may hold values from -1.25 to 1.25
- image_up: bfloat16 [768, 3072], P(None, 'mp'), may hold values from -0.21875 to 0.21875
- image_down: bfloat16 [3072, 768], P('mp'), may hold values from -0.109375 to 0.109375
- text_proj: bfloat16 [768, 2304], P(None, 'mp'), may hold values from -0.21875 to 0.21875
- text_mix: bfloat16 [768, 768], P('mp'), may hold values from -1.25 to 1.25
- cross_query: bfloat16 [768, 768], P(None, 'mp'), may hold values from -0.21875 to 0.21875
- cross_keyval: bfloat16 [768, 1536], P(None, 'mp'), may hold values from -0.21875 to 0.21875
- cross_mix: bfloat16 [768, 768], P('mp'), may hold values from -1.25 to 1.25
- text_up: bfloat16 [768, 3072], P(None, 'mp'), may hold values from -0.21875 to 0.21875
- text_down: bfloat16 [3072, 768], P('mp'), may hold values from -0.109375 to 0.109375
- image_cotan: bfloat16 [12544, 768], P(('dp', 'mp')), may hold values from -6 to 6
- text_cotan: bfloat16 [4096, 768], P(('dp', 'mp')), may hold values from -6 to 6
Outputs:
- image_embed: bfloat16 [12544, 768], P(('dp', 'mp'))
- text_embed: bfloat16 [4096, 768], P(('dp', 'mp'))
- grad_patches: bfloat16 [12544, 768], P(('dp', 'mp'))
- grad_captions: bfloat16 [4096, 768], P(('dp', 'mp'))
- grad_image_norm: float32 [768], replicated
- grad_image_ffnorm: float32 [768], replicated
- grad_text_norm: float32 [768], replicated
- grad_cross_norm: float32 [768], replicated
- grad_text_ffnorm: float32 [768], replicated
- grad_image_proj: float32 [768, 2304], P(None, 'mp')
- grad_image_mix: float32 [768, 768], P('mp')
- grad_image_up: float32 [768, 3072], P(None, 'mp')
- grad_image_down: float32 [3072, 768], P('mp')
- grad_text_proj: float32 [768, 2304], P(None, 'mp')
- grad_text_mix: float32 [768, 768], P('mp')
- grad_cross_query: float32 [768, 768], P(None, 'mp')
- grad_cross_keyval: float32 [768, 1536], P(None, 'mp')
- grad_cross_mix: float32 [768, 768], P('mp')
- grad_text_up: float32 [768, 3072], P(None, 'mp')
- grad_text_down: float32 [3072, 768], P('mp')
The draws below stay inside these ranges and needn't reach their ends.
Inputs may be any that keep to these rules, and one draw needn't show every extreme that they name: `patch_image`: the 784 rows of a group form 1 aligned blocks of 784 rows; each block holds one image of 784 patches or four images of 196 patches in a row; images are numbered from 0 up in row order within the group. `caption_image`: each caption names an image of its own group.
All inputs are finite; a program needn't handle non-finite values.
Results may differ from the reference program's by a relative error of at most 0.024.
Values may be sent and summed in bfloat16 or wider, within the bound.
A program may use at most 192 MiB of HBM per device.

```python
import jax
import jax.numpy as jnp
from jax import lax

D = 768
HEADS = 12
HD = 64
FF = 3072
LT = 128
IMG_LARGE = 784
IMG_SMALL = 196
BLOCKS = 1
CAPS = 2
CAP = 784
PATCHES = 12544
TEXT = 4096
N_DP = 16


def group_layout(key):
    layout_key = jax.random.fold_in(key, 11)
    large_flag = jax.random.randint(layout_key, (N_DP, BLOCKS), 0, 2)
    large_flag = large_flag.at[0].set(0)
    counts = large_flag + 4 * (1 - large_flag)
    offsets = jnp.cumsum(counts, axis=1) - counts
    position = jnp.arange(IMG_LARGE) // IMG_SMALL
    image_ids = offsets[:, :, None] + (1 - large_flag)[:, :, None] * position[None, None, :]
    return (image_ids.reshape(N_DP * BLOCKS * IMG_LARGE).astype(jnp.int32), jnp.sum(counts, axis=1))


def draw_patch_image(key, part):
    return group_layout(key)[0]


def draw_caption_image(key, part):
    image_ids, totals = group_layout(key)
    chosen = jax.random.randint(jax.random.fold_in(key, 23), (N_DP, CAPS), 0, totals[:, None])
    chosen = chosen.at[0, 0].set(0)
    chosen = chosen.at[0, CAPS - 1].set(4 * BLOCKS - 1)
    return chosen.reshape(N_DP * CAPS).astype(jnp.int32)


def level_of(own_key, extent, cuts, smallest, top_value):
    factor_of, own = 1.0, jax.random.fold_in(own_key, 6)
    for dim, shards_of in cuts:
        draws = jnp.exp(jax.random.uniform(jax.random.fold_in(own, dim), (shards_of,), jnp.float32, smallest / len(cuts), top_value / len(cuts)))
        factor_of = factor_of * jnp.repeat(draws, extent[dim] // shards_of).reshape([-1 if axis == dim else 1 for axis in range(len(extent))])
    return factor_of


def normal_values(own_key, dims, deviation, bound, shards=(), dtype=jnp.bfloat16):
    entries = jax.random.normal(own_key, dims, jnp.float32) * deviation
    if len(shards) > 0:
        entries = level_of(own_key, dims, shards, -0.22, 0.18) * entries
    return jnp.clip(entries, min=-bound, max=bound).astype(dtype)


def setup_inputs(seed: int = 0) -> dict:
    key_of = jax.random.split(jax.random.key(seed), 23)
    patches = normal_values(key_of[0], (PATCHES, D), 1.0, 6.0, ((0, 32),))
    captions = normal_values(key_of[1], (TEXT, D), 1.0, 6.0, ((0, 32),))
    patch_image = draw_patch_image(jax.random.fold_in(key_of[22], 71), 0)
    caption_image = draw_caption_image(jax.random.fold_in(key_of[22], 71), 0)
    image_norm = jnp.clip(1.0 + 0.1 * jax.random.normal(key_of[4], (D,), jnp.float32), 0.5, 1.5)
    image_ffnorm = jnp.clip(1.0 + 0.1 * jax.random.normal(key_of[5], (D,), jnp.float32), 0.5, 1.5)
    text_norm = jnp.clip(1.0 + 0.1 * jax.random.normal(key_of[6], (D,), jnp.float32), 0.5, 1.5)
    cross_norm = jnp.clip(1.0 + 0.1 * jax.random.normal(key_of[7], (D,), jnp.float32), 0.5, 1.5)
    text_ffnorm = jnp.clip(1.0 + 0.1 * jax.random.normal(key_of[8], (D,), jnp.float32), 0.5, 1.5)
    image_proj = normal_values(key_of[9], (D, 3 * D), D ** -0.5, 0.21875, ((1, 2),))
    image_mix = normal_values(key_of[10], (D, D), (D // 32) ** -0.5, 1.25, ((0, 2),))
    image_up = normal_values(key_of[11], (D, FF), D ** -0.5, 0.21875, ((1, 2),))
    image_down = normal_values(key_of[12], (FF, D), FF ** -0.5, 0.109375, ((0, 2),))
    text_proj = normal_values(key_of[13], (D, 3 * D), D ** -0.5, 0.21875, ((1, 2),))
    text_mix = normal_values(key_of[14], (D, D), (D // 32) ** -0.5, 1.25, ((0, 2),))
    cross_query = normal_values(key_of[15], (D, D), D ** -0.5, 0.21875, ((1, 2),))
    cross_keyval = normal_values(key_of[16], (D, 2 * D), D ** -0.5, 0.21875, ((1, 2),))
    cross_mix = normal_values(key_of[17], (D, D), (D // 32) ** -0.5, 1.25, ((0, 2),))
    text_up = normal_values(key_of[18], (D, FF), D ** -0.5, 0.21875, ((1, 2),))
    text_down = normal_values(key_of[19], (FF, D), FF ** -0.5, 0.109375, ((0, 2),))
    image_cotan = normal_values(key_of[20], (PATCHES, D), 1.0, 6.0, ((0, 32),))
    text_cotan = normal_values(key_of[21], (TEXT, D), 1.0, 6.0, ((0, 32),))
    return {"patches": patches, "captions": captions, "patch_image": patch_image, "caption_image": caption_image, "image_norm": image_norm, "image_ffnorm": image_ffnorm, "text_norm": text_norm, "cross_norm": cross_norm, "text_ffnorm": text_ffnorm, "image_proj": image_proj, "image_mix": image_mix, "image_up": image_up, "image_down": image_down, "text_proj": text_proj, "text_mix": text_mix, "cross_query": cross_query, "cross_keyval": cross_keyval, "cross_mix": cross_mix, "text_up": text_up, "text_down": text_down, "image_cotan": image_cotan, "text_cotan": text_cotan}


NEG_FILL = -1000000000.0
EPS = 1e-06
HIGHEST_PREC = lax.Precision.HIGHEST

@jax.custom_vjp
def low(v):
    return lax.optimization_barrier(v.astype(jnp.bfloat16)).astype(jnp.float32)

@jax.custom_vjp
def low_back(v):
    return v

def low_keep(v):
    return (low(v), None)

def low_pass(kept, grad):
    return (grad,)

def back_keep(v):
    return (v, None)

def back_low(kept, grad):
    return (low(grad),)
low.defvjp(low_keep, low_pass)
low_back.defvjp(back_keep, back_low)

def matmul(left, right):
    return jnp.dot(left, right, precision=HIGHEST_PREC)

def norm_rows(values, gain_vec):
    row_mean = lax.optimization_barrier(jnp.mean(values, axis=-1, keepdims=True))
    centred = values - row_mean
    row_var = lax.optimization_barrier(jnp.mean(centred * centred, axis=-1, keepdims=True))
    return centred * lax.rsqrt(row_var + EPS) * gain_vec

def attention(queries, key_rows, value_rows, allowed):
    factor = HD ** (-0.5)
    scores = low_back(factor * jnp.einsum('qhe,khe->hqk', queries, key_rows, precision=HIGHEST_PREC))
    scores = jnp.where(allowed[None], scores, NEG_FILL)
    probability = jax.nn.softmax(scores, axis=-1)
    return jnp.einsum('hqk,khe->qhe', low(probability), value_rows, precision=HIGHEST_PREC)

def gelu_exact(values):
    return jax.nn.gelu(values, approximate=False)

def group_forward(weights, patch_rows, caption_rows, image_ids, caption_ids):
    image_norm, image_ffnorm, text_norm, cross_norm, text_ffnorm, image_proj, image_mix, image_up, image_down, text_proj, text_mix, cross_query, cross_keyval, cross_mix, text_up, text_down = weights
    same_image = image_ids[:, None] == image_ids[None, :]
    position = jnp.arange(CAPS * LT)
    caption_index = position // LT
    causal = (caption_index[:, None] == caption_index[None, :]) & (position[None, :] <= position[:, None])
    row_image = caption_ids[caption_index]
    cross_allowed = row_image[:, None] == image_ids[None, :]
    normed = low(norm_rows(patch_rows, image_norm))
    head_rows = low(low_back(matmul(normed, image_proj))).reshape(CAP, HEADS, 3, HD)
    attended = attention(head_rows[:, :, 0], head_rows[:, :, 1], head_rows[:, :, 2], same_image)
    attended = low(low_back(attended.reshape(CAP, D)))
    image_mid = patch_rows + low_back(matmul(attended, image_mix))
    normed = low(norm_rows(image_mid, image_ffnorm))
    pre_act = low_back(matmul(normed, image_up))
    hidden = low(gelu_exact(pre_act))
    image_resid = image_mid + low_back(matmul(hidden, image_down))
    embed = low(image_resid)
    normed = low(norm_rows(caption_rows, text_norm))
    head_rows = low(low_back(matmul(normed, text_proj))).reshape(CAPS * LT, HEADS, 3, HD)
    attended = attention(head_rows[:, :, 0], head_rows[:, :, 1], head_rows[:, :, 2], causal)
    attended = low(low_back(attended.reshape(CAPS * LT, D)))
    text_mid = caption_rows + low_back(matmul(attended, text_mix))
    normed = low(norm_rows(text_mid, cross_norm))
    query_rows = low(low_back(matmul(normed, cross_query))).reshape(CAPS * LT, HEADS, HD)
    keyval_rows = low(low_back(matmul(embed, cross_keyval))).reshape(CAP, HEADS, 2, HD)
    attended = attention(query_rows, keyval_rows[:, :, 0], keyval_rows[:, :, 1], cross_allowed)
    attended = low(low_back(attended.reshape(CAPS * LT, D)))
    text_mid2 = text_mid + low_back(matmul(attended, cross_mix))
    normed = low(norm_rows(text_mid2, text_ffnorm))
    pre_act = low_back(matmul(normed, text_up))
    hidden = low(gelu_exact(pre_act))
    text_resid = text_mid2 + low_back(matmul(hidden, text_down))
    return (image_resid, text_resid)

def reference(patches, captions, patch_image, caption_image, image_norm, image_ffnorm, text_norm, cross_norm, text_ffnorm, image_proj, image_mix, image_up, image_down, text_proj, text_mix, cross_query, cross_keyval, cross_mix, text_up, text_down, image_cotan, text_cotan):
    weights = (image_norm.astype(jnp.float32), image_ffnorm.astype(jnp.float32), text_norm.astype(jnp.float32), cross_norm.astype(jnp.float32), text_ffnorm.astype(jnp.float32), image_proj.astype(jnp.float32), image_mix.astype(jnp.float32), image_up.astype(jnp.float32), image_down.astype(jnp.float32), text_proj.astype(jnp.float32), text_mix.astype(jnp.float32), cross_query.astype(jnp.float32), cross_keyval.astype(jnp.float32), cross_mix.astype(jnp.float32), text_up.astype(jnp.float32), text_down.astype(jnp.float32))
    patch_groups = patches.astype(jnp.float32).reshape(N_DP, CAP, D)
    caption_groups = captions.astype(jnp.float32).reshape(N_DP, CAPS * LT, D)
    image_ids = patch_image.reshape(N_DP, CAP)
    caption_ids = caption_image.reshape(N_DP, CAPS)

    def whole(weight_set, patch_set, caption_set):

        def one_group(pieces):
            return group_forward(weight_set, pieces[0], pieces[1], pieces[2], pieces[3])
        return lax.map(jax.checkpoint(one_group), (patch_set, caption_set, image_ids, caption_ids))
    outputs, pullback = jax.vjp(whole, weights, patch_groups, caption_groups)
    cotangents = (image_cotan.astype(jnp.float32).reshape(N_DP, CAP, D), text_cotan.astype(jnp.float32).reshape(N_DP, CAPS * LT, D))
    grad_weights, grad_patch_groups, grad_caption_groups = pullback(cotangents)
    return (outputs[0].reshape(N_DP * CAP, D).astype(jnp.bfloat16), outputs[1].reshape(N_DP * CAPS * LT, D).astype(jnp.bfloat16), grad_patch_groups.reshape(N_DP * CAP, D).astype(jnp.bfloat16), grad_caption_groups.reshape(N_DP * CAPS * LT, D).astype(jnp.bfloat16), grad_weights[0], grad_weights[1], grad_weights[2], grad_weights[3], grad_weights[4], grad_weights[5], grad_weights[6], grad_weights[7], grad_weights[8], grad_weights[9], grad_weights[10], grad_weights[11], grad_weights[12], grad_weights[13], grad_weights[14], grad_weights[15])
```

```python
import functools

import jax
import jax.numpy as jnp
from jax import lax
from jax.experimental import pallas as pl
from jax.experimental.pallas import tpu as pltpu
from jax.sharding import PartitionSpec as P

HD = 64
LT = 128
NEG_FILL = -1000000000.0
EPS = 1e-06
F32 = jnp.float32
BF16 = jnp.bfloat16
SCALE = HD**-0.5
VMEM_LIMIT = 56 * 2**20


def mm(left, right, left_dim, right_dim, **options):
    return lax.dot_general(
        left,
        right,
        (((left_dim,), (right_dim,)), ((), ())),
        preferred_element_type=F32,
        **options,
    )


def row_step(rows):
    return 112 if rows % 112 == 0 else 128


def over_rows(rows, body):
    step = row_step(rows)

    @pl.loop(0, rows // step)
    def _(i):
        body(pl.ds(pl.multiple_of(i * step, 16), step))


def norm_parts(values):
    centred = values - jnp.mean(values, axis=-1, keepdims=True)
    inv_std = lax.rsqrt(jnp.mean(centred * centred, axis=-1, keepdims=True) + EPS)
    return centred * inv_std, inv_std


def norm_back(grad_out, scaled, inv_std, gain):
    grad_scaled = grad_out * gain
    mean_grad = jnp.mean(grad_scaled, axis=-1, keepdims=True)
    mean_cross = jnp.mean(grad_scaled * scaled, axis=-1, keepdims=True)
    return inv_std * (grad_scaled - mean_grad - scaled * mean_cross)


def total(refs, rows):
    value = refs[0][rows].astype(F32)
    for ref in refs[1:]:
        value = value + ref[rows].astype(F32)
    return value


def gelu_both(values):
    half = 0.5 * (1.0 + lax.erf(values * (0.5**0.5)))
    density = jnp.exp(-0.5 * values * values) * ((0.5 / jnp.pi) ** 0.5)
    return values * half, half + values * density


def allowed_of(key_ref, query_ref, causal):
    allowed = key_ref[...] == query_ref[...]
    if causal:
        key_row = lax.broadcasted_iota(jnp.int32, allowed.shape, 0)
        query_row = lax.broadcasted_iota(jnp.int32, allowed.shape, 1)
        allowed = allowed & (key_row <= query_row)
    return allowed


def attend_pair(heads, allowed, lse_ref):
    outs = []
    for h, (query, key, value) in enumerate(heads):
        scores = jnp.where(allowed, mm(key, query, 1, 1), NEG_FILL)
        top = jnp.max(scores, axis=0, keepdims=True)
        weight = jnp.exp(scores - top).astype(BF16)
        with_ones = jnp.concatenate((value, jnp.ones(value.shape, BF16)), axis=1)
        result = mm(with_ones, weight, 0, 0)
        sums = result[HD : HD + 1]
        outs.append(result[:HD] / sums)
        lse_ref[0, h : h + 1] = top + jnp.log(sums)
    return jnp.concatenate(outs, axis=0).T.astype(BF16)


def attend_pair_back(heads, allowed, lse_ref, att, grad_att):
    product = grad_att.astype(F32) * att.astype(F32)
    lane = lax.broadcasted_iota(jnp.int32, (8, 2 * HD), 1)
    line = lax.broadcasted_iota(jnp.int32, (8, 2 * HD), 0)
    pick = jnp.where(lane // HD == line, 1.0, 0.0).astype(F32)
    row_dots = mm(pick, product, 1, 1, precision=lax.Precision.HIGHEST)
    grad_queries, rest = [], []
    for h, (query, key, value) in enumerate(heads):
        grad_head = grad_att[:, h * HD : (h + 1) * HD]
        scores = jnp.where(allowed, mm(key, query, 1, 1), NEG_FILL)
        prob = jnp.exp(scores - lse_ref[0, h : h + 1])
        grad_value = mm(prob.astype(BF16), grad_head, 1, 0)
        grad_prob = mm(value, grad_head, 1, 1)
        grad_scores = (prob * (grad_prob - row_dots[h : h + 1])).astype(BF16)
        rest.append((mm(grad_scores, query, 1, 0), grad_value))
        grad_queries.append(mm(key, grad_scores, 0, 0))
    return jnp.concatenate(grad_queries, axis=0).T * SCALE, rest


def split_heads(block):
    factor = jnp.asarray(SCALE, BF16)
    heads = []
    for h in range(2):
        query, key, value = (
            block[:, (3 * h + j) * HD : (3 * h + j + 1) * HD] for j in range(3)
        )
        heads.append((query * factor, key, value))
    return heads


def split_cross(query_block, keyval_block):
    factor = jnp.asarray(SCALE, BF16)
    return [
        (
            query_block[:, h * HD : (h + 1) * HD] * factor,
            keyval_block[:, 2 * h * HD : (2 * h + 1) * HD],
            keyval_block[:, (2 * h + 1) * HD : (2 * h + 2) * HD],
        )
        for h in range(2)
    ]


def whole(shape):
    return pl.BlockSpec(shape, lambda i: (0,) * len(shape), pipeline_mode=pl.Buffered(1))


def columns(rows, width):
    return pl.BlockSpec((rows, width), lambda i: (0, i))


def lines(height, width):
    return pl.BlockSpec((height, width), lambda i: (i, 0))


def per_pair(rows):
    return pl.BlockSpec((1, 2, rows), lambda i: (i, 0, 0))


def out(shape, dtype):
    return jax.ShapeDtypeStruct(shape, dtype)


def call(kernel, name, steps, ins, outs, scratch, args, flops):
    size = sum(a.size * a.dtype.itemsize for a in args)
    size += sum(o.size * o.dtype.itemsize for o, _ in outs)
    return pl.pallas_call(
        kernel,
        name=name,
        grid=(steps,),
        in_specs=ins,
        out_specs=[spec for _, spec in outs],
        out_shape=[shape for shape, _ in outs],
        scratch_shapes=scratch,
        compiler_params=pltpu.CompilerParams(vmem_limit_bytes=VMEM_LIMIT),
        cost_estimate=pl.CostEstimate(flops=flops, bytes_accessed=size, transcendentals=0),
    )(*args)


def self_forward(rows_in, gain, proj, mix, ids, causal, name):
    rows, width = rows_in.shape
    pairs = mix.shape[0] // (2 * HD)

    def kernel(x, g, w, m, kid, qid, normed, qkv, att, lse, part, acc):
        step = pl.program_id(0)

        @pl.when(step == 0)
        def _():
            def body(at):
                scaled, _ = norm_parts(x[at].astype(F32))
                normed[at] = (scaled * g[...]).astype(BF16)

            over_rows(rows, body)

        block = mm(normed[...], w[...], 1, 0).astype(BF16)
        qkv[...] = block
        result = attend_pair(split_heads(block), allowed_of(kid, qid, causal), lse)
        att[...] = result
        share = mm(result, m[...], 1, 0)

        @pl.when(step == 0)
        def _():
            acc[...] = share

        @pl.when((step > 0) & (step < pairs - 1))
        def _():
            acc[...] += share

        @pl.when(step == pairs - 1)
        def _():
            part[...] = (acc[...] + share).astype(BF16)

    flops = 2 * rows * (width * (4 * pairs * 2 * HD) + rows * pairs * 4 * HD)
    return call(
        kernel,
        name,
        pairs,
        [
            whole((rows, width)),
            whole((1, width)),
            columns(width, 6 * HD),
            lines(2 * HD, width),
            whole((rows, 1)),
            whole((1, rows)),
        ],
        [
            (out((rows, width), BF16), whole((rows, width))),
            (out((rows, pairs * 6 * HD), BF16), columns(rows, 6 * HD)),
            (out((rows, pairs * 2 * HD), BF16), columns(rows, 2 * HD)),
            (out((pairs, 2, rows), F32), per_pair(rows)),
            (out((rows, width), BF16), whole((rows, width))),
        ],
        [pltpu.VMEM((rows, width), F32)],
        (rows_in, gain.reshape(1, width), proj, mix, ids.reshape(rows, 1), ids.reshape(1, rows)),
        flops,
    )


def feed_forward(pieces, gain, up, down, name):
    rows, width = pieces[0].shape
    hidden = up.shape[1]
    block = 256
    steps = hidden // block
    count = len(pieces)

    def kernel(*refs):
        parts = refs[:count]
        g, u, d, mid, normed, hid, slope, part, acc = refs[count:]
        step = pl.program_id(0)

        @pl.when(step == 0)
        def _():
            def body(at):
                value = total(parts, at)
                mid[at] = value
                scaled, _ = norm_parts(value)
                normed[at] = (scaled * g[...]).astype(BF16)

            over_rows(rows, body)

        value, derivative = gelu_both(mm(normed[...], u[...], 1, 0))
        value = value.astype(BF16)
        hid[...] = value
        slope[...] = derivative.astype(BF16)
        share = mm(value, d[...], 1, 0)

        @pl.when(step == 0)
        def _():
            acc[...] = share

        @pl.when((step > 0) & (step < steps - 1))
        def _():
            acc[...] += share

        @pl.when(step == steps - 1)
        def _():
            part[...] = (acc[...] + share).astype(BF16)

    return call(
        kernel,
        name,
        steps,
        [whole((rows, width))] * count
        + [whole((1, width)), columns(width, block), lines(block, width)],
        [
            (out((rows, width), F32), whole((rows, width))),
            (out((rows, width), BF16), whole((rows, width))),
            (out((rows, hidden), BF16), columns(rows, block)),
            (out((rows, hidden), BF16), columns(rows, block)),
            (out((rows, width), BF16), whole((rows, width))),
        ],
        [pltpu.VMEM((rows, width), F32)],
        (*pieces, gain.reshape(1, width), up, down),
        4 * rows * width * hidden,
    )


def cross_forward(image_pieces, text_pieces, gain, query_w, keyval_w, mix, key_id, query_id):
    keys, width = image_pieces[0].shape
    rows = text_pieces[0].shape[0]
    pairs = mix.shape[0] // (2 * HD)
    n_image, n_text = len(image_pieces), len(text_pieces)

    def kernel(*refs):
        image = refs[:n_image]
        text = refs[n_image : n_image + n_text]
        g, wq, wkv, m, kid, qid = refs[n_image + n_text : n_image + n_text + 6]
        embed, mid, normed, q, kv, att, lse, part, acc = refs[n_image + n_text + 6 :]
        step = pl.program_id(0)

        @pl.when(step == 0)
        def _():
            def image_body(at):
                embed[at] = total(image, at).astype(BF16)

            over_rows(keys, image_body)

            def text_body(at):
                value = total(text, at)
                mid[at] = value
                scaled, _ = norm_parts(value)
                normed[at] = (scaled * g[...]).astype(BF16)

            over_rows(rows, text_body)

        query_block = mm(normed[...], wq[...], 1, 0).astype(BF16)
        keyval_block = mm(embed[...], wkv[...], 1, 0).astype(BF16)
        q[...] = query_block
        kv[...] = keyval_block
        result = attend_pair(
            split_cross(query_block, keyval_block), allowed_of(kid, qid, False), lse
        )
        att[...] = result
        share = mm(result, m[...], 1, 0)

        @pl.when(step == 0)
        def _():
            acc[...] = share

        @pl.when((step > 0) & (step < pairs - 1))
        def _():
            acc[...] += share

        @pl.when(step == pairs - 1)
        def _():
            part[...] = (acc[...] + share).astype(BF16)

    flops = 2 * pairs * 2 * HD * (width * (2 * rows + 2 * keys) + 2 * rows * keys)
    return call(
        kernel,
        "cross_forward",
        pairs,
        [whole((keys, width))] * n_image
        + [whole((rows, width))] * n_text
        + [
            whole((1, width)),
            columns(width, 2 * HD),
            columns(width, 4 * HD),
            lines(2 * HD, width),
            whole((keys, 1)),
            whole((1, rows)),
        ],
        [
            (out((keys, width), BF16), whole((keys, width))),
            (out((rows, width), F32), whole((rows, width))),
            (out((rows, width), BF16), whole((rows, width))),
            (out((rows, pairs * 2 * HD), BF16), columns(rows, 2 * HD)),
            (out((keys, pairs * 4 * HD), BF16), columns(keys, 4 * HD)),
            (out((rows, pairs * 2 * HD), BF16), columns(rows, 2 * HD)),
            (out((pairs, 2, rows), F32), per_pair(rows)),
            (out((rows, width), BF16), whole((rows, width))),
        ],
        [pltpu.VMEM((rows, width), F32)],
        (
            *image_pieces,
            *text_pieces,
            gain.reshape(1, width),
            query_w,
            keyval_w,
            mix,
            key_id.reshape(keys, 1),
            query_id.reshape(1, rows),
        ),
        flops,
    )


def feed_both(pieces, cotan, gain, up, down):
    rows, width = pieces[0].shape
    hidden = up.shape[1]
    block = 256
    steps = hidden // block
    count = len(pieces)

    def kernel(*refs):
        parts = refs[:count]
        gy, g, u, d, mid, normed, hid, dpre, part, dpart, acc, dacc = refs[count:]
        step = pl.program_id(0)

        @pl.when(step == 0)
        def _():
            def body(at):
                value = total(parts, at)
                mid[at] = value
                scaled, _ = norm_parts(value)
                normed[at] = (scaled * g[...]).astype(BF16)

            over_rows(rows, body)
            acc[...] = jnp.zeros_like(acc)
            dacc[...] = jnp.zeros_like(dacc)

        value, derivative = gelu_both(mm(normed[...], u[...], 1, 0))
        value = value.astype(BF16)
        hid[...] = value
        acc[...] += mm(value, d[...], 1, 0)
        grad_pre = (mm(gy[...], d[...], 1, 1) * derivative).astype(BF16)
        dpre[...] = grad_pre
        dacc[...] += mm(grad_pre, u[...], 1, 1)

        @pl.when(step == steps - 1)
        def _():
            part[...] = acc[...].astype(BF16)
            dpart[...] = dacc[...].astype(BF16)

    return call(
        kernel,
        "text_feed",
        steps,
        [whole((rows, width))] * (count + 1)
        + [whole((1, width)), columns(width, block), lines(block, width)],
        [
            (out((rows, width), F32), whole((rows, width))),
            (out((rows, width), BF16), whole((rows, width))),
            (out((rows, hidden), BF16), columns(rows, block)),
            (out((rows, hidden), BF16), columns(rows, block)),
            (out((rows, width), BF16), whole((rows, width))),
            (out((rows, width), BF16), whole((rows, width))),
        ],
        [pltpu.VMEM((rows, width), F32)] * 2,
        (*pieces, cotan, gain.reshape(1, width), up, down),
        8 * rows * width * hidden,
    )


def norm_back_rows(rows, grads, mid, gain, upper, grad_sum, grad_low, gain_grad):
    gain_grad[...] = jnp.zeros_like(gain_grad)

    def body(at):
        grad = total(grads, at)
        scaled, inv_std = norm_parts(mid[at])
        gain_grad[...] += jnp.sum(grad * scaled, axis=0, keepdims=True)
        value = total(upper, at) + norm_back(grad, scaled, inv_std, gain[...])
        grad_sum[at] = value
        grad_low[at] = value.astype(BF16)

    over_rows(rows, body)


def cross_back(upper, grads, mid, gain, q, kv, att, lse, query_w, keyval_w, mix, key_id, query_id):
    rows, width = mid.shape
    keys = kv.shape[0]
    pairs = mix.shape[0] // (2 * HD)

    def kernel(up0, g0, g1, md, g, qr, kvr, ar, lr, wq, wkv, m, kid, qid, *rest):
        gsum, glow, ggain, dq, dkv, dpart, epart, dacc, eacc = rest
        step = pl.program_id(0)

        @pl.when(step == 0)
        def _():
            norm_back_rows(rows, (g0, g1), md, g, (up0,), gsum, glow, ggain)
            dacc[...] = jnp.zeros_like(dacc)
            eacc[...] = jnp.zeros_like(eacc)

        grad_att = mm(glow[...], m[...], 1, 1).astype(BF16)
        grad_query, rest_pair = attend_pair_back(
            split_cross(qr[...], kvr[...]), allowed_of(kid, qid, False), lr, ar[...], grad_att
        )
        grad_query = grad_query.astype(BF16)
        dq[...] = grad_query
        grad_keyval = jnp.concatenate([piece for pair in rest_pair for piece in pair], axis=1)
        grad_keyval = grad_keyval.astype(BF16)
        dkv[...] = grad_keyval
        dacc[...] += mm(grad_query, wq[...], 1, 1)
        eacc[...] += mm(grad_keyval, wkv[...], 1, 1)

        @pl.when(step == pairs - 1)
        def _():
            dpart[...] = dacc[...].astype(BF16)
            epart[...] = eacc[...].astype(BF16)

    flops = 2 * pairs * 2 * HD * (width * (2 * rows + 2 * keys) + 5 * rows * keys)
    return call(
        kernel,
        "cross_back",
        pairs,
        [whole((rows, width))] * 4
        + [
            whole((1, width)),
            columns(rows, 2 * HD),
            columns(keys, 4 * HD),
            columns(rows, 2 * HD),
            per_pair(rows),
            columns(width, 2 * HD),
            columns(width, 4 * HD),
            lines(2 * HD, width),
            whole((keys, 1)),
            whole((1, rows)),
        ],
        [
            (out((rows, width), F32), whole((rows, width))),
            (out((rows, width), BF16), whole((rows, width))),
            (out((1, width), F32), whole((1, width))),
            (out(q.shape, BF16), columns(rows, 2 * HD)),
            (out(kv.shape, BF16), columns(keys, 4 * HD)),
            (out((rows, width), BF16), whole((rows, width))),
            (out((keys, width), BF16), whole((keys, width))),
        ],
        [pltpu.VMEM((rows, width), F32), pltpu.VMEM((keys, width), F32)],
        (
            upper,
            *grads,
            mid,
            gain.reshape(1, width),
            q,
            kv,
            att,
            lse,
            query_w,
            keyval_w,
            mix,
            key_id.reshape(keys, 1),
            query_id.reshape(1, rows),
        ),
        flops,
    )


def self_back(upper, grads, mid, gain, qkv, att, lse, proj, mix, ids, causal, rows_in, name):
    rows, width = mid.shape
    pairs = mix.shape[0] // (2 * HD)

    def kernel(up0, g0, g1, md, g, qr, ar, lr, w, m, kid, qid, x, *rest):
        gsum, glow, ggain, dqkv, dpart, igain, dacc = rest
        step = pl.program_id(0)

        @pl.when(step == 0)
        def _():
            norm_back_rows(rows, (g0, g1), md, g, (up0,), gsum, glow, ggain)
            dacc[...] = jnp.zeros_like(dacc)

        grad_att = mm(glow[...], m[...], 1, 1).astype(BF16)
        grad_query, pair = attend_pair_back(
            split_heads(qr[...]), allowed_of(kid, qid, causal), lr, ar[...], grad_att
        )
        grad_block = jnp.concatenate(
            [grad_query[:, :HD], *pair[0], grad_query[:, HD:], *pair[1]], axis=1
        ).astype(BF16)
        dqkv[...] = grad_block
        dacc[...] += mm(grad_block, w[...], 1, 1)

        @pl.when(step == pairs - 1)
        def _():
            igain[...] = jnp.zeros_like(igain)

            def body(at):
                grad = dacc[at]
                scaled, _ = norm_parts(x[at].astype(F32))
                igain[...] += jnp.sum(grad * scaled, axis=0, keepdims=True)
                dpart[at] = grad.astype(BF16)

            over_rows(rows, body)

    flops = 2 * rows * pairs * 2 * HD * (width * 4 + 5 * rows)
    return call(
        kernel,
        name,
        pairs,
        [whole((rows, width))] * 4
        + [
            whole((1, width)),
            columns(rows, 6 * HD),
            columns(rows, 2 * HD),
            per_pair(rows),
            columns(width, 6 * HD),
            lines(2 * HD, width),
            whole((rows, 1)),
            whole((1, rows)),
            whole((rows, width)),
        ],
        [
            (out((rows, width), F32), whole((rows, width))),
            (out((rows, width), BF16), whole((rows, width))),
            (out((1, width), F32), whole((1, width))),
            (out(qkv.shape, BF16), columns(rows, 6 * HD)),
            (out((rows, width), BF16), whole((rows, width))),
            (out((1, width), F32), whole((1, width))),
        ],
        [pltpu.VMEM((rows, width), F32)],
        (
            upper,
            *grads,
            mid,
            gain.reshape(1, width),
            qkv,
            att,
            lse,
            proj,
            mix,
            ids.reshape(rows, 1),
            ids.reshape(1, rows),
            rows_in,
        ),
        flops,
    )


def feed_back(pieces, slope, up, down):
    rows, width = pieces[0].shape
    hidden = up.shape[1]
    block = 256
    steps = hidden // block
    count = len(pieces)

    def kernel(*refs):
        parts = refs[:count]
        sl, u, d, gsum, glow, dpre, dpart, dacc = refs[count:]
        step = pl.program_id(0)

        @pl.when(step == 0)
        def _():
            def body(at):
                value = total(parts, at)
                gsum[at] = value
                glow[at] = value.astype(BF16)

            over_rows(rows, body)

        grad_pre = (mm(glow[...], d[...], 1, 1) * sl[...].astype(F32)).astype(BF16)
        dpre[...] = grad_pre
        share = mm(grad_pre, u[...], 1, 1)

        @pl.when(step == 0)
        def _():
            dacc[...] = share

        @pl.when((step > 0) & (step < steps - 1))
        def _():
            dacc[...] += share

        @pl.when(step == steps - 1)
        def _():
            dpart[...] = (dacc[...] + share).astype(BF16)

    return call(
        kernel,
        "image_feed_back",
        steps,
        [whole((rows, width))] * count
        + [columns(rows, block), columns(width, block), lines(block, width)],
        [
            (out((rows, width), F32), whole((rows, width))),
            (out((rows, width), BF16), whole((rows, width))),
            (out((rows, hidden), BF16), columns(rows, block)),
            (out((rows, width), BF16), whole((rows, width))),
        ],
        [pltpu.VMEM((rows, width), F32)],
        (*pieces, slope, up, down),
        4 * rows * width * hidden,
    )


def local(
    patches,
    captions,
    patch_image,
    caption_image,
    image_norm,
    image_ffnorm,
    text_norm,
    cross_norm,
    text_ffnorm,
    image_proj,
    image_mix,
    image_up,
    image_down,
    text_proj,
    text_mix,
    cross_query,
    cross_keyval,
    cross_mix,
    text_up,
    text_down,
    image_cotan,
    text_cotan,
):
    side = lax.axis_index("mp")
    place = lax.axis_index("dp")
    ring = lax.axis_size("dp")
    image_own = patches.shape[0]
    text_own = captions.shape[0]
    text_rows = 2 * text_own

    def swap(rows):
        return lax.ppermute(rows, "mp", [(0, 1), (1, 0)])

    def both(own_rows):
        other = swap(own_rows)
        return jnp.where(
            side == 0,
            jnp.concatenate((own_rows, other), axis=0),
            jnp.concatenate((other, own_rows), axis=0),
        )

    def own_half(rows, own):
        return lax.dynamic_slice_in_dim(rows, side * own, own)

    def partner(bit):
        return [(i, i ^ (1 << bit)) for i in range(ring)]

    levels = [bit for bit in range(4) if 2 << bit <= ring]

    def reduce_pairs(rows):
        for bit in levels:
            half = rows.shape[0] // 2
            mine = (place >> bit) & 1
            got = lax.ppermute(
                lax.dynamic_slice_in_dim(rows, (1 - mine) * half, half), "dp", partner(bit)
            )
            keep = lax.dynamic_slice_in_dim(rows, mine * half, half)
            rows = (keep.astype(F32) + got.astype(F32)).astype(BF16)
        if ring > 1 << len(levels):
            size = 1 << len(levels)
            groups = [list(range(first, ring, size)) for first in range(size)]
            rows = lax.psum(rows, "dp", axis_index_groups=groups)
        for bit in reversed(levels):
            mine = (place >> bit) & 1
            got = lax.ppermute(rows, "dp", partner(bit))
            rows = jnp.where(
                mine == 0,
                jnp.concatenate((rows, got), axis=0),
                jnp.concatenate((got, rows), axis=0),
            )
        return rows.astype(F32)

    def reduce_all(value):
        value = value + swap(value)
        bit = 0
        while 1 << bit < ring:
            value = value + lax.ppermute(value, "dp", partner(bit))
            bit += 1
        return value

    def weight_grad(left, right):
        return mm(left, right, 0, 0).astype(BF16)

    def stacked(*pieces):
        width = patches.shape[1]
        flat = []
        for piece in pieces:
            if piece.shape[1] < width:
                cut = piece.shape[0] * piece.shape[1] // width
                flat.append(jnp.concatenate((piece[:cut], piece[cut:]), axis=1))
            elif piece.shape[1] % width:
                body = piece.shape[1] // width * width
                flat += [piece[:, i : i + width] for i in range(0, body, width)]
                rest = piece[:, body:]
                cut = rest.shape[0] * rest.shape[1] // width
                flat.append(jnp.concatenate((rest[:cut], rest[cut:]), axis=1))
            else:
                flat += [piece[:, i : i + width] for i in range(0, piece.shape[1], width)]
        return jnp.concatenate(flat, axis=0)

    def unstacked(rows, shapes):
        width = patches.shape[1]
        found, at = [], 0

        def take(count):
            nonlocal at
            at += count
            return rows[at - count : at]

        for height, across in shapes:
            parts = [take(height) for _ in range(across // width)]
            rest = across % width
            if rest:
                cut = take(height * rest // width)
                parts.append(jnp.concatenate((cut[:, :rest], cut[:, rest:]), axis=0))
            found.append(parts[0] if len(parts) == 1 else jnp.concatenate(parts, axis=1))
        return found

    def reduce_stage(*pieces):
        return unstacked(reduce_pairs(stacked(*pieces)), [piece.shape for piece in pieces])

    caption_of = jnp.arange(text_rows, dtype=jnp.int32) // LT
    row_image = jnp.broadcast_to(caption_image[:, None], (caption_image.shape[0], LT))
    row_image = row_image.reshape(text_rows)

    patch_all = both(patches)
    caption_all = both(captions)
    text_cotan_all = both(text_cotan)
    image_cotan_all = both(image_cotan)

    normed_one, image_qkv, image_att, image_lse, mix_part = self_forward(
        patch_all, image_norm, image_proj, image_mix, patch_image, False, "image_self"
    )
    mix_got = swap(mix_part)
    normed_three, text_qkv, text_att, text_lse, text_part = self_forward(
        caption_all, text_norm, text_proj, text_mix, caption_of, True, "text_self"
    )
    text_got = swap(text_part)
    image_mid, normed_two, image_hidden, image_slope, down_part = feed_forward(
        (patch_all, mix_part, mix_got), image_ffnorm, image_up, image_down, "image_feed"
    )
    down_got = swap(down_part)
    (
        embed_all,
        text_mid,
        normed_four,
        cross_q,
        cross_kv,
        cross_att,
        cross_lse,
        cross_part,
    ) = cross_forward(
        (image_mid, down_part, down_got),
        (caption_all, text_part, text_got),
        cross_norm,
        cross_query,
        cross_keyval,
        cross_mix,
        patch_image,
        row_image,
    )
    cross_got = swap(cross_part)
    text_mid2, normed_five, text_hidden, text_dpre, text_down_part, text_dpart = feed_both(
        (text_mid, cross_part, cross_got), text_cotan_all, text_ffnorm, text_up, text_down
    )
    text_dgot = swap(text_dpart)
    text_low = swap(
        lax.dynamic_slice_in_dim(text_down_part, (1 - side) * text_own, text_own)
    )
    text_embed = (
        own_half(text_mid2, text_own)
        + own_half(text_down_part, text_own).astype(F32)
        + text_low.astype(F32)
    ).astype(BF16)
    text_up_grad = weight_grad(normed_five, text_dpre)
    text_down_grad = weight_grad(text_hidden, text_cotan_all)

    (
        grad_mid2,
        grad_mid2_low,
        gain_five,
        dcross_q,
        dcross_kv,
        cross_dpart,
        embed_dpart,
    ) = cross_back(
        text_cotan_all,
        (text_dpart, text_dgot),
        text_mid2,
        text_ffnorm,
        cross_q,
        cross_kv,
        cross_att,
        cross_lse,
        cross_query,
        cross_keyval,
        cross_mix,
        patch_image,
        row_image,
    )
    embed_dgot = swap(embed_dpart)
    cross_dgot = swap(cross_dpart)
    grad_resid, grad_resid_low, image_dpre, feed_dpart = feed_back(
        (image_cotan_all, embed_dpart, embed_dgot), image_slope, image_up, image_down
    )
    feed_dgot = swap(feed_dpart)
    grad_mid, grad_mid_low, gain_four, dtext_qkv, text_dlast, gain_three = self_back(
        grad_mid2,
        (cross_dpart, cross_dgot),
        text_mid,
        cross_norm,
        text_qkv,
        text_att,
        text_lse,
        text_proj,
        text_mix,
        caption_of,
        True,
        caption_all,
        "text_self_back",
    )
    image_up_grad = weight_grad(normed_two, image_dpre)
    image_down_grad = weight_grad(image_hidden, grad_resid_low)
    (
        grad_image_mid,
        grad_image_low,
        gain_two,
        dimage_qkv,
        image_dlast,
        gain_one,
    ) = self_back(
        grad_resid,
        (feed_dpart, feed_dgot),
        image_mid,
        image_ffnorm,
        image_qkv,
        image_att,
        image_lse,
        image_proj,
        image_mix,
        patch_image,
        False,
        patch_all,
        "image_self_back",
    )

    def input_grad(grad_rows, partial_rows, rows_in, gain, own):
        got = swap(lax.dynamic_slice_in_dim(partial_rows, (1 - side) * own, own))
        grad = own_half(partial_rows, own).astype(F32) + got.astype(F32)
        scaled, inv_std = norm_parts(rows_in.astype(F32))
        back = norm_back(grad, scaled, inv_std, gain)
        return (own_half(grad_rows, own) + back).astype(BF16)

    grad_patches = input_grad(grad_image_mid, image_dlast, patches, image_norm, image_own)
    grad_captions = input_grad(grad_mid, text_dlast, captions, text_norm, text_own)

    text_up_sum, text_down_sum = reduce_stage(text_up_grad, text_down_grad)
    mid_sums = reduce_stage(
        weight_grad(normed_three, dtext_qkv),
        weight_grad(text_att, grad_mid_low),
        weight_grad(normed_four, dcross_q),
        weight_grad(embed_all, dcross_kv),
        weight_grad(cross_att, grad_mid2_low),
    )
    image_up_sum, image_down_sum = reduce_stage(image_up_grad, image_down_grad)
    image_proj_sum, image_mix_sum = reduce_stage(
        weight_grad(normed_one, dimage_qkv), weight_grad(image_att, grad_image_low)
    )
    gains = reduce_all(
        jnp.concatenate(
            (gain_one, 0.5 * gain_two, gain_three, 0.5 * gain_four, 0.5 * gain_five), axis=0
        )
    )
    return (
        own_half(embed_all, image_own),
        text_embed,
        grad_patches,
        grad_captions,
        gains[0],
        gains[1],
        gains[2],
        gains[3],
        gains[4],
        image_proj_sum,
        image_mix_sum,
        image_up_sum,
        image_down_sum,
        *mid_sums,
        text_up_sum,
        text_down_sum,
    )


def solution(mesh):
    return jax.shard_map(
        local,
        mesh=mesh,
        in_specs=(
            P(("dp", "mp"), None),
            P(("dp", "mp"), None),
            P("dp"),
            P("dp"),
            P(),
            P(),
            P(),
            P(),
            P(),
            P(None, "mp"),
            P("mp", None),
            P(None, "mp"),
            P("mp", None),
            P(None, "mp"),
            P("mp", None),
            P(None, "mp"),
            P(None, "mp"),
            P("mp", None),
            P(None, "mp"),
            P("mp", None),
            P(("dp", "mp"), None),
            P(("dp", "mp"), None),
        ),
        out_specs=(
            P(("dp", "mp"), None),
            P(("dp", "mp"), None),
            P(("dp", "mp"), None),
            P(("dp", "mp"), None),
            P(),
            P(),
            P(),
            P(),
            P(),
            P(None, "mp"),
            P("mp", None),
            P(None, "mp"),
            P("mp", None),
            P(None, "mp"),
            P("mp", None),
            P(None, "mp"),
            P(None, "mp"),
            P("mp", None),
            P(None, "mp"),
            P("mp", None),
        ),
        check_vma=False,
    )
```
